16 devices in a mesh: dp: 4 (over y, z, core), tp: 4 (over x).
Axes of the slice: x: 4, y: 2, z: 1, core: 2. Of those that a mesh axis runs over, the one named last changes fastest.
The devices are a block of a 4x4x4 slice.
Arguments:
- x: bfloat16 [8192, 8192], P('dp'), parts along dimension 0
- w_gate: bfloat16 [8192, 32768], P(None, 'tp')
- w_up: bfloat16 [8192, 32768], P(None, 'tp')
- w_down: bfloat16 [32768, 8192], P('tp')
Outputs:
- output: bfloat16 [8192, 8192], P('dp'), parts along dimension 0
There are 4 independent parts. The reference program is written for one: setup_inputs(seed, part) draws one part's arguments, and reference() takes and returns one part's arrays. A program takes and returns all parts, laid end to end along the dimension named above; an argument that names none is the same for every part.
All inputs are finite; a program needn't handle non-finite values.
Results may differ from the reference program's by a relative error of at most 0.016.
Values are sent between devices in bfloat16 or wider.
A program may use at most 1.5 GiB of HBM per device.

```python
import jax
import jax.numpy as jnp

ROWS = 2048
D = 8192
FF = 32768


def setup_inputs(seed: int = 0, part: int = 0) -> dict:
    kx, kg, ku, kd = jax.random.split(jax.random.key(seed), 4)
    drawn = {
        "x": jax.random.normal(jax.random.fold_in(kx, part), (ROWS, D), jnp.float32),
        "w_gate": jax.random.normal(kg, (D, FF), jnp.float32) * D**-0.5,
        "w_up": jax.random.normal(ku, (D, FF), jnp.float32) * D**-0.5,
        "w_down": jax.random.normal(kd, (FF, D), jnp.float32) * FF**-0.5,
    }
    return {k: v.astype(jnp.bfloat16) for k, v in drawn.items()}


def reference(x, w_gate, w_up, w_down):
    gate = jnp.dot(x, w_gate, preferred_element_type=jnp.float32)
    up = jnp.dot(x, w_up, preferred_element_type=jnp.float32)
    hidden = (jax.nn.silu(gate) * up).astype(jnp.bfloat16)
    return jnp.dot(hidden, w_down, preferred_element_type=jnp.float32).astype(jnp.bfloat16)
```

```python
import functools

import jax
import jax.numpy as jnp
from jax import lax
from jax.experimental import pallas as pl
from jax.experimental.pallas import tpu as pltpu
from jax.sharding import PartitionSpec as P

MESH = pl.DeviceIdType.MESH
BF16, F32 = jnp.bfloat16, jnp.float32
COL = 256
SLOTS = 4
STAGE = 4
RING = 6
SENDS = 4
LARGE, COUNT = 448, 4


def products(lhs, wv, slot):
    K = wv.shape[2]
    out = [None, None]
    for k in range(K // COL):
        at = pl.ds(k * COL, COL)
        a = lhs(at)
        for i in range(2):
            v = jnp.dot(a, wv[slot, i, at, :], preferred_element_type=F32)
            out[i] = v if k == 0 else out[i] + v
    return out


def kernel(nt, large, count, x, wg, wu, wd, y, xv, hv, wv, rsin, stg, wsem, xsem, rssend, rsrecv, credit, agrecv, agsend, lsem):
    rows, K = x.shape
    small = rows - large * count
    part = y.shape[1] // (2 * nt)
    nb = part // COL
    dn, gn = nt * nb, wg.shape[1] // COL
    drounds, rounds = dn // 2, gn // 2
    phase = dn + gn
    total = gn + count * phase + dn
    rsn = dn - nb

    me = lax.axis_index("tp")
    right, left = lax.rem(me + 1, nt), lax.rem(me + nt - 1, nt)
    ahead, behind = (right, left), (left, right)

    barrier = pltpu.get_barrier_semaphore()
    for other in (left, right):
        pl.semaphore_signal(barrier, inc=1, device_id={"tp": other}, device_id_type=MESH)
    pl.semaphore_wait(barrier, 2)

    def col_of(way, hop, b):
        owner = lax.rem(me - hop + nt, nt) if way == 0 else lax.rem(me + hop, nt)
        return pl.multiple_of(way * (part * nt) + owner * part + b * COL, COL)

    def w_start(t):
        slot = lax.rem(t, SLOTS)
        rho = lax.rem(jnp.maximum(t - gn, 0), phase)
        q, r = rho // 4, lax.rem(rho, 4)
        last = t >= gn + count * phase
        down = last | ((t >= gn) & (rho < 4 * drounds) & (r < 2))
        ds = jnp.where(last, t - gn - count * phase, 2 * q + r)
        j = jnp.where(t < gn, t, jnp.where(rho < 4 * drounds, 2 * q + r - 2, rho - dn))

        @pl.when(down & (t < total))
        def _():
            a, b = ds // nb, lax.rem(ds, nb)
            for way in range(2):
                src = wd.at[:, pl.ds(col_of(way, a + 1, b), COL)]
                pltpu.make_async_copy(src, wv.at[slot, way], wsem.at[slot, way]).start()

        @pl.when(jnp.logical_not(down))
        def _():
            c = pl.ds(pl.multiple_of(j * COL, COL), COL)
            for i, w in enumerate((wg, wu)):
                pltpu.make_async_copy(w.at[:, c], wv.at[slot, i], wsem.at[slot, i]).start()

    def w_wait(t):
        slot = lax.rem(t, SLOTS)
        for i in range(2):
            pltpu.make_async_copy(wg.at[:, pl.ds(0, COL)], wv.at[slot, i], wsem.at[slot, i]).wait()

    def x_copy(row, m):
        return pltpu.make_async_copy(x.at[pl.ds(row, m), :], xv.at[pl.ds(0, m), :], xsem)

    def rs_copy(way, m, s, slot):
        return pltpu.make_async_remote_copy(
            src_ref=stg.at[way, s, pl.ds(0, m)], dst_ref=rsin.at[way, slot, pl.ds(0, m)],
            send_sem=rssend.at[way, s], recv_sem=rsrecv.at[way, slot],
            device_id={"tp": ahead[way]}, device_id_type=MESH)

    def y_at(way, hop, row, m, b):
        return y.at[pl.ds(row, m), pl.ds(col_of(way, hop, b), COL)]

    def y_own(way, m, s, row, b):
        return pltpu.make_async_copy(stg.at[way, s, pl.ds(0, m)], y_at(way, 0, row, m, b), lsem.at[way, s])

    def ag_first(way, m, s, row, b, c):
        return pltpu.make_async_remote_copy(
            src_ref=stg.at[way, s, pl.ds(0, m)], dst_ref=y_at(way, 0, row, m, b),
            send_sem=rssend.at[way, s], recv_sem=agrecv.at[way, 0, c * nb + b],
            device_id={"tp": ahead[way]}, device_id_type=MESH)

    def ag_copy(way, hop, m, row, b, c, f, recv):
        at = y_at(way, hop, row, m, b)
        return pltpu.make_async_remote_copy(
            src_ref=at, dst_ref=at, send_sem=agsend.at[way, f], recv_sem=agrecv.at[way, recv, c * nb + b],
            device_id={"tp": ahead[way]}, device_id_type=MESH)

    def forward(c, row, m, ev, m_before):
        hop, b = 1 + ev // nb, lax.rem(ev, nb)
        n = c * (nt - 2) * nb + ev
        f = lax.rem(n, SENDS)

        @pl.when(n >= SENDS)
        def _():
            for way in range(2):
                ag_copy(way, 1, m_before, 0, 0, 0, f, 0).wait_send()

        for way in range(2):
            ag_copy(way, hop, m, row, b, c, f, hop - 1).wait_recv()
            ag_copy(way, hop, m, row, b, c, f, hop).start()

    def gate_up(m, t, n, hs, j):
        for k in range(n):
            w_wait(t + k)
        for k in range(n):
            slot = lax.rem(t + k, SLOTS)
            g, u = products(lambda at: xv[pl.ds(0, m), at], wv, slot)
            at = pl.ds(pl.multiple_of((j + k) * COL, COL), COL)
            hv[hs, pl.ds(0, m), at] = (jax.nn.silu(g) * u).astype(BF16)
        for k in range(n):
            w_start(t + SLOTS + k)

    def down(m, t, n, hs, c, ds, m_before):
        for k in range(n):
            w_wait(t + k)
        dc = c * dn + ds

        @pl.when(dc >= STAGE)
        def _():
            for k in range(n):
                s = lax.rem(dc + k, STAGE)
                for way in range(2):
                    rs_copy(way, m_before, s, 0).wait_send()

        @pl.when((c >= 1) & (ds < nb))
        def _():
            for k in range(n):
                s = lax.rem(dc + k, STAGE)
                for way in range(2):
                    y_own(way, m_before, s, 0, 0).wait()

        @pl.when(ds >= nb)
        def _():
            for k in range(n):
                for way in range(2):
                    rs_copy(way, m, 0, lax.rem(c * rsn + ds - nb + k, RING)).wait_recv()

        for k in range(n):
            slot, s = lax.rem(t + k, SLOTS), lax.rem(dc + k, STAGE)
            came = jnp.where(ds >= nb, lax.rem(jnp.maximum(c * rsn + ds - nb + k, 0), RING), RING)
            both = products(lambda at: hv[hs, pl.ds(0, m), at], wv, slot)
            for way in range(2):
                v = both[way]
                v = v + rsin[way, came, pl.ds(0, m), :].astype(F32)
                stg[way, s, pl.ds(0, m), :] = v.astype(BF16)
        for k in range(n):
            w_start(t + SLOTS + k)

    def send(m, n, c, row, ds):
        dc, so = c * dn + ds, c * rsn + ds

        @pl.when((ds >= nb) & (so - nb + RING < (count + 1) * rsn))
        def _():
            for way in range(2):
                for k in range(n):
                    @pl.when(so - nb + k + RING < (count + 1) * rsn)
                    def _():
                        pl.semaphore_signal(credit.at[way], inc=1, device_id={"tp": behind[way]}, device_id_type=MESH)

        @pl.when(ds < rsn)
        def _():
            for k in range(n):
                @pl.when(so + k >= RING)
                def _():
                    for way in range(2):
                        pl.semaphore_wait(credit.at[way], 1)

                for way in range(2):
                    rs_copy(way, m, lax.rem(dc + k, STAGE), lax.rem(so + k, RING)).start()

        @pl.when(ds >= rsn)
        def _():
            for k in range(n):
                s, b = lax.rem(dc + k, STAGE), ds - rsn + k
                for way in range(2):
                    ag_first(way, m, s, row, b, c).start()
                    y_own(way, m, s, row, b).start()

    def row_of(c):
        return pl.multiple_of(c * large, 16)

    x_copy(0, large).start()
    for s in range(SLOTS):
        w_start(jnp.int32(s))
    rsin[:, RING] = jnp.zeros_like(rsin[:, RING])
    x_copy(0, large).wait()

    def large_round(n, _):
        i, q = n // rounds, lax.rem(n, rounds)
        t = jnp.where(i == 0, 2 * q, gn + (i - 1) * phase + jnp.where(q < drounds, 4 * q, dn + 2 * q))
        has_down = (i > 0) & (q < drounds)

        @pl.when((i > 0) & (q == 0))
        def _():
            x_copy(row_of(i), large).start()

        @pl.when(has_down)
        def _():
            down(large, t, 2, lax.rem(i + 1, 2), i - 1, 2 * q, large)
            send(large, 2, i - 1, row_of(i - 1), 2 * q)

        @pl.when((i > 0) & (q == 0))
        def _():
            x_copy(row_of(i), large).wait()

        @pl.when((i > 0) & (q >= drounds) & (q - drounds < (nt - 2) * nb))
        def _():
            forward(i - 1, row_of(i - 1), large, q - drounds, large)

        gate_up(large, jnp.where(has_down, t + 2, t), 2, lax.rem(i, 2), 2 * q)
        return 0

    lax.fori_loop(0, count * rounds, large_round, 0)

    t0, c0 = gn + (count - 1) * phase, count - 1
    hs0, hs1 = c0 % 2, count % 2
    x_copy(count * large, small).start()

    def small_round(q, _):
        t = t0 + jnp.where(q < drounds, 4 * q, dn + 2 * q)

        @pl.when(q < drounds)
        def _():
            down(large, t, 2, hs0, c0, 2 * q, large)
            send(large, 2, c0, c0 * large, 2 * q)

        @pl.when(q == 0)
        def _():
            x_copy(count * large, small).wait()

        @pl.when((q >= drounds) & (q - drounds < (nt - 2) * nb))
        def _():
            forward(c0, c0 * large, large, q - drounds, large)

        def one(k, _):
            gate_up(small, jnp.where(q < drounds, t + 2, t) + k, 1, hs1, 2 * q + k)
            return 0

        lax.fori_loop(0, 2, one, 0)
        return 0

    lax.fori_loop(0, rounds, small_round, 0)

    def last_round(ds, _):
        t = t0 + phase + ds
        first = nb

        @pl.when(ds < first)
        def _():
            before(ds, large)

        @pl.when(ds >= first)
        def _():
            before(ds, small)

        down_last(t, ds)
        send(small, 1, count, count * large, ds)
        return 0

    def before(ds, m):
        s = lax.rem(count * dn + ds, STAGE)
        for way in range(2):
            rs_copy(way, m, s, 0).wait_send()

    def down_last(t, ds):
        w_wait(t)
        c = count
        dc = c * dn + ds
        slot, s = lax.rem(t, SLOTS), lax.rem(dc, STAGE)

        @pl.when(ds < nb)
        def _():
            for way in range(2):
                y_own(way, large, s, 0, 0).wait()

        @pl.when(ds >= nb)
        def _():
            for way in range(2):
                rs_copy(way, small, 0, lax.rem(c * rsn + ds - nb, RING)).wait_recv()

        came = jnp.where(ds >= nb, lax.rem(c * rsn + ds - nb, RING), RING)
        both = products(lambda at: hv[hs1, pl.ds(0, small), at], wv, slot)
        for way in range(2):
            v = both[way]
            v = v + rsin[way, came, pl.ds(0, small), :].astype(F32)
            stg[way, s, pl.ds(0, small), :] = v.astype(BF16)
        w_start(t + SLOTS)

    lax.fori_loop(0, dn, last_round, 0)

    for ev in range((nt - 2) * nb):
        forward(count, count * large, small, jnp.int32(ev), large if ev < SENDS else small)
    for b in range(nb):
        s = (count * dn + rsn + b) % STAGE
        for way in range(2):
            rs_copy(way, small, s, 0).wait_send()
            y_own(way, small, s, 0, 0).wait()
    for f in range(SENDS):
        for way in range(2):
            ag_copy(way, 1, small, 0, 0, 0, f, 0).wait_send()
    for c in range(count + 1):
        m = large if c < count else small
        for b in range(nb):
            for way in range(2):
                ag_copy(way, nt - 1, m, c * large, b, c, 0, nt - 2).wait_recv()


def block(nt, large, count, x, wg, wu, wd):
    rows, K = x.shape
    nb = wd.shape[1] // (2 * nt * COL)
    assert STAGE == nb and (nt - 2) * nb >= SENDS and wg.shape[1] == K and wd.shape[0] == K
    return pl.pallas_call(
        functools.partial(kernel, nt, large, count),
        out_shape=jax.ShapeDtypeStruct((rows, wd.shape[1]), BF16),
        in_specs=[pl.BlockSpec(memory_space=pl.ANY)] * 4,
        out_specs=pl.BlockSpec(memory_space=pl.ANY),
        scratch_shapes=[
            pltpu.VMEM((large, K), BF16),
            pltpu.VMEM((2, large, K), BF16),
            pltpu.VMEM((SLOTS, 2, K, COL), BF16),
            pltpu.VMEM((2, RING + 1, large, COL), BF16),
            pltpu.VMEM((2, STAGE, large, COL), BF16),
            pltpu.SemaphoreType.DMA((SLOTS, 2)),
            pltpu.SemaphoreType.DMA,
            pltpu.SemaphoreType.DMA((2, STAGE)),
            pltpu.SemaphoreType.DMA((2, RING)),
            pltpu.SemaphoreType.REGULAR((2,)),
            pltpu.SemaphoreType.DMA((2, nt - 1, (count + 1) * nb)),
            pltpu.SemaphoreType.DMA((2, SENDS)),
            pltpu.SemaphoreType.DMA((2, STAGE)),
        ],
        compiler_params=pltpu.CompilerParams(collective_id=0, has_side_effects=True, vmem_limit_bytes=67043328),
        name="mlp_block",
    )(x, wg, wu, wd)


def solution(mesh):
    nt = mesh.shape["tp"]
    return jax.shard_map(
        functools.partial(block, nt, LARGE, COUNT),
        mesh=mesh,
        in_specs=(P("dp", None), P(None, "tp"), P(None, "tp"), P("tp", None)),
        out_specs=P("dp", None),
        check_vma=False,
    )
```

```python
import functools

import jax
import jax.numpy as jnp
from jax import lax
from jax.experimental import pallas as pl
from jax.experimental.pallas import tpu as pltpu
from jax.sharding import PartitionSpec as P

MESH = pl.DeviceIdType.MESH
BF16, F32 = jnp.bfloat16, jnp.float32
COL = 256
WIDE = 2 * COL
SLOTS = 4
LARGE, COUNT = 448, 4


def kernel(nt, large, count, x, wg, wu, wd, y, wv, xv, hv, rsin, stg, wsem, xsem,
           rssend, rsrecv, agrecv, agsend, lsem, srssend, srsrecv, sagrecv, sagsend, slsem, vsem):
    rows, K = x.shape
    small = rows - large * count
    part = y.shape[1] // (2 * nt)
    nb = part // COL
    lag = nb // 2
    ring = 2 * lag
    dn, gn = nt * nb, wg.shape[1] // COL
    drounds = dn // 2
    phase = dn + gn
    total = gn + count * phase + dn
    rsn = drounds - lag
    hops = nt - 1

    me = lax.axis_index("tp")
    right, left = lax.rem(me + 1, nt), lax.rem(me + nt - 1, nt)
    ahead = (right, left)

    def col_of(way, hop, c):
        owner = lax.rem(me - hop + 2 * nt, nt) if way == 0 else lax.rem(me + hop, nt)
        return pl.multiple_of(way * (part * nt) + owner * part + c, COL)

    def w_start(t):
        slot = lax.rem(t, SLOTS)
        u = jnp.maximum(t - gn, 0)
        i = jnp.minimum(u // phase, count)
        rho = u - i * phase
        turn = jnp.where(i == count - 1, 3, 4)
        q, last = rho // turn, i == count
        r = rho - q * turn
        mixed = q < drounds
        down = last | ((t >= gn) & mixed & (r < 2))
        ds = jnp.minimum(jnp.where(last, rho, 2 * q + r), dn - 1)
        j = jnp.where(t < gn, t, jnp.where(mixed, (turn - 2) * q + r - 2, rho - dn))

        @pl.when(down & (t <= total))
        def _():
            a, b = ds // nb, lax.rem(ds, nb)
            for way in range(2):
                src = wd.at[:, pl.ds(col_of(way, a + 1, b * COL), COL)]
                pltpu.make_async_copy(src, wv.at[slot, way], wsem.at[slot, way]).start()

        @pl.when(jnp.logical_not(down))
        def _():
            c = pl.ds(pl.multiple_of(j * COL, COL), COL)
            for i, w in enumerate((wg, wu)):
                pltpu.make_async_copy(w.at[:, c], wv.at[slot, i], wsem.at[slot, i]).start()

    def w_wait(t):
        slot = lax.rem(t, SLOTS)
        for i in range(2):
            pltpu.make_async_copy(wg.at[:, pl.ds(0, COL)], wv.at[slot, i], wsem.at[slot, i]).wait()

    def x_copy(row, m):
        return pltpu.make_async_copy(x.at[pl.ds(row, m), :], xv.at[pl.ds(0, m), :], xsem)

    def remote(way, src, dst, send_sem, recv_sem):
        return pltpu.make_async_remote_copy(
            src_ref=src, dst_ref=dst, send_sem=send_sem, recv_sem=recv_sem,
            device_id={"tp": ahead[way]}, device_id_type=MESH)

    def rs_copy(way, s, slot):
        return remote(way, stg.at[way, s], rsin.at[way, slot], rssend.at[way, s], rsrecv.at[way, slot])

    def y_at(way, hop, c, f):
        return y.at[pl.ds(pl.multiple_of(c * large, 16), large), pl.ds(col_of(way, hop, f * WIDE), WIDE)]

    def y_own(way, s, c, f):
        return pltpu.make_async_copy(stg.at[way, s], y_at(way, 0, c, f), lsem.at[way, s])

    def ag_first(way, s, c, f):
        return remote(way, stg.at[way, s], y_at(way, 0, c, f), rssend.at[way, s], agrecv.at[way, 0, c * lag + f])

    def ag_copy(way, hop, c, f, s, recv):
        at = y_at(way, hop, c, f)
        return remote(way, at, at, agsend.at[way, s], agrecv.at[way, recv, c * lag + f])

    def forward(c, ev, on):
        hop, f = 1 + ev // lag, lax.rem(ev, lag)
        n = c * (nt - 2) * lag + ev
        s = lax.rem(n, 2)
        for way in range(2):
            @pl.when(on & (n >= 2))
            def _():
                ag_copy(way, 1, 0, 0, s, 0).wait_send()

            @pl.when(on)
            def _():
                ag_copy(way, hop, c, f, s, hop - 1).wait_recv()

            @pl.when(on)
            def _():
                ag_copy(way, hop, c, f, s, hop).start()

    def half(h):
        return pl.ds(pl.multiple_of(h * COL, COL), COL)

    def small_rs(way, s, h, slot):
        return remote(way, stg.at[way, s, pl.ds(0, small), half(h)], rsin.at[way, slot, pl.ds(0, small), half(h)],
                      srssend.at[way, 2 * s + h], srsrecv.at[way, 2 * slot + h])

    def small_y(way, hop, b):
        return y.at[pl.ds(large * count, small), pl.ds(col_of(way, hop, b * COL), COL)]

    def small_own(way, s, h, b):
        return pltpu.make_async_copy(stg.at[way, s, pl.ds(0, small), half(h)], small_y(way, 0, b), slsem.at[way, 2 * s + h])

    def small_first(way, s, h, b):
        return remote(way, stg.at[way, s, pl.ds(0, small), half(h)], small_y(way, 0, b),
                      srssend.at[way, 2 * s + h], sagrecv.at[way, 0, b])

    def small_ag(way, hop, b, s, recv):
        at = small_y(way, hop, b)
        return remote(way, at, at, sagsend.at[way, s], sagrecv.at[way, recv, b])

    def products(lhs, t, beside):
        slot = lax.rem(t, SLOTS)
        beside = [(K // COL // 4, lambda: w_start(t + 3)), (3 * (K // COL) // 4, lambda: w_wait(t + 1)), *beside]
        out = [None, None]
        for k in range(K // COL):
            at = pl.ds(k * COL, COL)
            a = lhs(at)
            for i in range(2):
                v = jnp.dot(a, wv[slot, i, at, :], preferred_element_type=F32)
                out[i] = v if k == 0 else out[i] + v
            for when, act in beside:
                if when == k:
                    act()
        return out

    mid = K // COL // 2

    def gate_up(m, t, hs, j, *beside):
        g, u = products(lambda at: xv[pl.ds(0, m), at], t, beside)
        hv[hs, pl.ds(0, m), pl.ds(pl.multiple_of(j * COL, COL), COL)] = (jax.nn.silu(g) * u).astype(BF16)

    def down_pair(t, hs, c, q, beside):
        s = lax.rem(c * drounds + q, lag)
        came = lax.rem(jnp.maximum(c * rsn + q - lag, 0), ring)
        place = jnp.where(q >= lag, came, ring)

        def ready():
            for way in range(2):
                @pl.when(c * drounds + q >= lag)
                def _():
                    rs_copy(way, s, 0).wait_send()

                @pl.when((c >= 1) & (q < lag))
                def _():
                    y_own(way, s, 0, 0).wait()

                @pl.when(q >= lag)
                def _():
                    rs_copy(way, 0, came).wait_recv()

        for k in range(2):
            both = products(lambda at: hv[hs, :, at], t + k, [(mid, ready)] if k == 0 else beside)
            at = pl.ds(k * COL, COL)
            for way in range(2):
                v = both[way] + rsin[way, place, :, at].astype(F32)
                stg[way, s, :, at] = v.astype(BF16)

    def send(c, q):
        s = lax.rem(c * drounds + q, lag)
        slot = lax.rem(c * rsn + q, ring)
        for way in range(2):
            @pl.when(q < rsn)
            def _():
                rs_copy(way, s, slot).start()

            @pl.when(q >= rsn)
            def _():
                ag_first(way, s, c, q - rsn).start()

            @pl.when(q >= rsn)
            def _():
                y_own(way, s, c, q - rsn).start()

    w_start(jnp.int32(0))
    x_copy(0, large).start()
    barrier = pltpu.get_barrier_semaphore()
    for other in (left, right):
        pl.semaphore_signal(barrier, inc=1, device_id={"tp": other}, device_id_type=MESH)
    pl.semaphore_wait(barrier, 2)
    w_start(jnp.int32(1))
    rsin[:, ring] = jnp.zeros_like(rsin[:, ring])
    x_copy(0, large).wait()
    w_wait(jnp.int32(0))
    w_start(jnp.int32(2))

    first, each = gn // 4, phase // 4

    def large_steps(v, _):
        i = jnp.where(v < first, 0, 1 + (v - first) // each)
        z = jnp.where(v < first, v + drounds, lax.rem(jnp.maximum(v - first, 0), each))
        t = 4 * v
        hs = lax.rem(i, 2)

        @pl.when(z < drounds)
        def _():
            @pl.when(z == 0)
            def _():
                x_copy(pl.multiple_of(i * large, 16), large).start()

            def x_wait():
                pl.when(z == 0)(lambda: x_copy(0, large).wait())

            down_pair(t, 1 - hs, i - 1, z, [(mid, x_wait)])
            gate_up(large, t + 2, hs, 2 * z, (mid, lambda: send(i - 1, z)))
            gate_up(large, t + 3, hs, 2 * z + 1)

        @pl.when(z >= drounds)
        def _():
            j = jnp.where(v < first, 4 * v, 4 * z - dn)
            ev = z - drounds
            on = (v >= first) & (ev < (nt - 2) * lag)
            gate_up(large, t, hs, j, (mid, lambda: forward(i - 1, ev, on)))
            for k in range(1, 4):
                gate_up(large, t + k, hs, j + k)

        return 0

    lax.fori_loop(0, first + each * (count - 1), large_steps, 0)

    t0, c0 = gn + (count - 1) * phase, count - 1
    hs0, hs1 = c0 % 2, count % 2
    x_copy(count * large, small).start()

    def mixed_steps(q, _):
        t = t0 + 3 * q

        def x_wait():
            pl.when(q == 0)(lambda: x_copy(0, small).wait())

        down_pair(t, hs0, c0, q, [(mid, x_wait)])
        gate_up(small, t + 2, hs1, q, (mid, lambda: send(c0, q)))
        return 0

    lax.fori_loop(0, drounds, mixed_steps, 0)

    def small_steps(n, _):
        j = drounds + 2 * n
        on = (lax.rem(n, 3) == 0) & (n // 3 < (nt - 2) * lag)
        gate_up(small, t0 + dn + j, hs1, j, (mid, lambda: forward(c0, n // 3, on)))
        gate_up(small, t0 + dn + j + 1, hs1, j + 1)
        return 0

    lax.fori_loop(0, (gn - drounds) // 2, small_steps, 0)

    t0 += phase

    def last_steps(ds, _):
        q, h = ds // 2, lax.rem(ds, 2)
        s = lax.rem(count * drounds + q, lag)
        came = lax.rem(count * rsn + jnp.maximum(q - lag, 0), ring)
        place = jnp.where(ds >= nb, came, ring)

        def ready():
            for way in range(2):
                @pl.when((q < lag) & (h == 0))
                def _():
                    rs_copy(way, s, 0).wait_send()
                    y_own(way, s, 0, 0).wait()

                @pl.when(ds >= nb)
                def _():
                    small_rs(way, s, h, 0).wait_send()

                @pl.when(ds >= nb)
                def _():
                    small_rs(way, 0, h, came).wait_recv()

        both = products(lambda at: hv[hs1, pl.ds(0, small), at], t0 + ds, [(3 * mid // 2, ready)])
        for way in range(2):
            v = both[way] + rsin[way, place, pl.ds(0, small), half(h)].astype(F32)
            stg[way, s, pl.ds(0, small), half(h)] = v.astype(BF16)
        slot, b = lax.rem(count * rsn + q, ring), ds - 2 * rsn

        @pl.when(ds < 2 * rsn)
        def _():
            for way in range(2):
                small_rs(way, s, h, slot).start()

        @pl.when(ds >= 2 * rsn)
        def _():
            for way in range(2):
                small_first(way, s, h, b).start()
                small_own(way, s, h, b).start()

        return 0

    lax.fori_loop(0, dn, last_steps, 0)

    for n in range(count * lag):
        for way in range(2):
            ag_copy(way, hops, n // lag, n % lag, 0, hops - 1).wait_recv()

    def keep(b):
        src = y.at[pl.ds(0, large * count), pl.ds(b * COL, COL)]
        return pltpu.make_async_copy(src, column(wv, b, large * count, rows), vsem.at[b])

    for b in range(y.shape[1] // COL):
        keep(b).start()

    for ev in range((nt - 2) * nb):
        hop, b = 1 + ev // nb, ev % nb
        for way in range(2):
            if ev >= nb:
                small_ag(way, 1, 0, b, 0).wait_send()
            small_ag(way, hop, b, b, hop - 1).wait_recv()
            small_ag(way, hop, b, b, hop).start()
    for way in range(2):
        for b in range(nb):
            small_rs(way, b // 2, b % 2, 0).wait_send()
            small_own(way, b // 2, b % 2, 0).wait()
            small_ag(way, 1, 0, b, 0).wait_send()
        for s in range(2):
            ag_copy(way, 1, 0, 0, s, 0).wait_send()
    for b in range(y.shape[1] // COL):
        keep(b).wait()
    for way in range(2):
        for b in range(nb):
            small_ag(way, hops, b, 0, hops - 1).wait_recv()


def column(v, b, rows, whole):
    per = v.shape[2] // whole
    return v.at[b // (2 * per), (b // per) % 2, pl.ds(b % per * whole, rows), :]


def lay_out(done, y, v, out, tail, sem, sems):
    rows, n = out.shape[0], out.shape[1] // COL
    rest = pltpu.make_async_copy(y.at[pl.ds(done, rows - done), :], tail, sem)
    rest.start()

    def copy(b):
        return pltpu.make_async_copy(column(v, b, done, rows), out.at[pl.ds(0, done), pl.ds(b * COL, COL)], sems.at[b])

    for b in range(n):
        copy(b).start()
    rest.wait()
    rest = pltpu.make_async_copy(tail, out.at[pl.ds(done, rows - done), :], sem)
    rest.start()
    for b in range(n):
        copy(b).wait()
    rest.wait()


def block(nt, large, count, x, wg, wu, wd):
    rows, K = x.shape
    nb = wd.shape[1] // (2 * nt * COL)
    lag = nb // 2
    assert wg.shape[1] == K and wd.shape[0] == K and wd.shape[1] == K and count * (nt - 2) * lag >= 2
    dma = pltpu.SemaphoreType.DMA
    y, v = pl.pallas_call(
        functools.partial(kernel, nt, large, count),
        out_shape=[jax.ShapeDtypeStruct((rows, wd.shape[1]), BF16), pltpu.VMEM((SLOTS, 2, K, COL), BF16)],
        in_specs=[pl.BlockSpec(memory_space=pl.ANY)] * 4,
        out_specs=[pl.BlockSpec(memory_space=pl.ANY), pl.BlockSpec(memory_space=pltpu.VMEM)],
        scratch_shapes=[
            pltpu.VMEM((large, K), BF16),
            pltpu.VMEM((2, large, K), BF16),
            pltpu.VMEM((2, 2 * lag + 1, large, WIDE), BF16),
            pltpu.VMEM((2, lag, large, WIDE), BF16),
            dma((SLOTS, 2)), dma,
            dma((2, lag)), dma((2, 2 * lag)), dma((2, nt - 1, count * lag)), dma((2, 2)), dma((2, lag)),
            dma((2, nb)), dma((2, 2 * nb)), dma((2, nt - 1, nb)), dma((2, nb)), dma((2, nb)), dma((wd.shape[1] // COL,)),
        ],
        compiler_params=pltpu.CompilerParams(collective_id=0, has_side_effects=True, vmem_limit_bytes=30 * 2**20),
        name="mlp_block",
    )(x, wg, wu, wd)
    return pl.pallas_call(
        functools.partial(lay_out, large * count),
        out_shape=jax.ShapeDtypeStruct((rows, wd.shape[1]), BF16),
        in_specs=[pl.BlockSpec(memory_space=pl.ANY)] * 2,
        out_specs=pl.BlockSpec(memory_space=pl.ANY),
        scratch_shapes=[pltpu.VMEM((rows - large * count, wd.shape[1]), BF16), dma, dma((wd.shape[1] // COL,))],
        compiler_params=pltpu.CompilerParams(vmem_limit_bytes=8 * 2**20),
        name="lay_out",
    )(pltpu.with_memory_space_constraint(y, pltpu.HBM), pltpu.with_memory_space_constraint(v, pltpu.VMEM))


def solution(mesh):
    nt = mesh.shape["tp"]
    return jax.shard_map(
        functools.partial(block, nt, LARGE, COUNT),
        mesh=mesh,
        in_specs=(P("dp", None), P(None, "tp"), P(None, "tp"), P("tp", None)),
        out_specs=P("dp", None),
        check_vma=False,
    )
```

```python
import functools

import jax
import jax.numpy as jnp
from jax import lax
from jax.experimental import pallas as pl
from jax.experimental.pallas import tpu as pltpu
from jax.sharding import PartitionSpec as P

MESH = pl.DeviceIdType.MESH
BF16, F32 = jnp.bfloat16, jnp.float32
COL = 256
WIDE = 2 * COL
SLOTS = 4
LARGE, COUNT = 448, 4


def kernel(nt, large, count, x, wg, wu, wd, y, wv, xv, hv, rsin, stg, wsem, xsem,
           rssend, rsrecv, agrecv, agsend, lsem, srssend, srsrecv, sagrecv, sagsend, slsem, vsem):
    rows, K = x.shape
    small = rows - large * count
    part = y.shape[1] // (2 * nt)
    nb = part // COL
    lag = nb // 2
    ring = 2 * lag
    dn, gn = nt * nb, wg.shape[1] // COL
    drounds = dn // 2
    phase = dn + gn
    total = gn + count * phase + dn
    rsn = drounds - lag
    hops = nt - 1

    me = lax.axis_index("tp")
    right, left = lax.rem(me + 1, nt), lax.rem(me + nt - 1, nt)
    ahead = (right, left)

    def col_of(way, hop, c):
        owner = lax.rem(me - hop + 2 * nt, nt) if way == 0 else lax.rem(me + hop, nt)
        return pl.multiple_of(way * (part * nt) + owner * part + c, COL)

    def w_start(t):
        slot = lax.rem(t, SLOTS)
        u = jnp.maximum(t - gn, 0)
        i = jnp.minimum(u // phase, count)
        rho = u - i * phase
        turn = jnp.where(i == count - 1, 3, 4)
        q, last = rho // turn, i == count
        r = rho - q * turn
        mixed = q < drounds
        down = last | ((t >= gn) & mixed & (r < 2))
        ds = jnp.minimum(jnp.where(last, rho, 2 * q + r), dn - 1)
        j = jnp.where(t < gn, t, jnp.where(mixed, (turn - 2) * q + r - 2, rho - dn))

        @pl.when(down & (t <= total))
        def _():
            a, b = ds // nb, lax.rem(ds, nb)
            for way in range(2):
                src = wd.at[:, pl.ds(col_of(way, a + 1, b * COL), COL)]
                pltpu.make_async_copy(src, wv.at[slot, way], wsem.at[slot, way]).start()

        @pl.when(jnp.logical_not(down))
        def _():
            c = pl.ds(pl.multiple_of(j * COL, COL), COL)
            for i, w in enumerate((wg, wu)):
                pltpu.make_async_copy(w.at[:, c], wv.at[slot, i], wsem.at[slot, i]).start()

    def w_wait(t):
        slot = lax.rem(t, SLOTS)
        for i in range(2):
            pltpu.make_async_copy(wg.at[:, pl.ds(0, COL)], wv.at[slot, i], wsem.at[slot, i]).wait()

    def x_copy(row, m):
        return pltpu.make_async_copy(x.at[pl.ds(row, m), :], xv.at[pl.ds(0, m), :], xsem)

    def remote(way, src, dst, send_sem, recv_sem):
        return pltpu.make_async_remote_copy(
            src_ref=src, dst_ref=dst, send_sem=send_sem, recv_sem=recv_sem,
            device_id={"tp": ahead[way]}, device_id_type=MESH)

    def rs_copy(way, s, slot):
        return remote(way, stg.at[way, s], rsin.at[way, slot], rssend.at[way, s], rsrecv.at[way, slot])

    def y_at(way, hop, c, f):
        return y.at[pl.ds(pl.multiple_of(c * large, 16), large), pl.ds(col_of(way, hop, f * WIDE), WIDE)]

    def y_own(way, s, c, f):
        return pltpu.make_async_copy(stg.at[way, s], y_at(way, 0, c, f), lsem.at[way, s])

    def ag_first(way, s, c, f):
        return remote(way, stg.at[way, s], y_at(way, 0, c, f), rssend.at[way, s], agrecv.at[way, 0, c * lag + f])

    def ag_copy(way, hop, c, f, s, recv):
        at = y_at(way, hop, c, f)
        return remote(way, at, at, agsend.at[way, s], agrecv.at[way, recv, c * lag + f])

    def forward(c, ev, on):
        hop, f = 1 + ev // lag, lax.rem(ev, lag)
        n = c * (nt - 2) * lag + ev
        s = lax.rem(n, 2)
        for way in range(2):
            @pl.when(on & (n >= 2))
            def _():
                ag_copy(way, 1, 0, 0, s, 0).wait_send()

            @pl.when(on)
            def _():
                ag_copy(way, hop, c, f, s, hop - 1).wait_recv()

            @pl.when(on)
            def _():
                ag_copy(way, hop, c, f, s, hop).start()

    def half(h):
        return pl.ds(pl.multiple_of(h * COL, COL), COL)

    def small_rs(way, s, h, slot):
        return remote(way, stg.at[way, s, pl.ds(0, small), half(h)], rsin.at[way, slot, pl.ds(0, small), half(h)],
                      srssend.at[way, 2 * s + h], srsrecv.at[way, 2 * slot + h])

    def small_y(way, hop, b):
        return y.at[pl.ds(large * count, small), pl.ds(col_of(way, hop, b * COL), COL)]

    def small_own(way, s, h, b):
        return pltpu.make_async_copy(stg.at[way, s, pl.ds(0, small), half(h)], small_y(way, 0, b), slsem.at[way, 2 * s + h])

    def small_first(way, s, h, b):
        return remote(way, stg.at[way, s, pl.ds(0, small), half(h)], small_y(way, 0, b),
                      srssend.at[way, 2 * s + h], sagrecv.at[way, 0, b])

    def small_ag(way, hop, b, s, recv):
        at = small_y(way, hop, b)
        return remote(way, at, at, sagsend.at[way, s], sagrecv.at[way, recv, b])

    def products(lhs, t, waits, beside):
        slot = lax.rem(t, SLOTS)
        beside = [(1, lambda: w_start(t + 3)), *((late, functools.partial(w_wait, t + 1 + n)) for n in range(waits)), *((late, act) for act in beside)]
        out = [None, None]
        for k in range(K // COL):
            at = pl.ds(k * COL, COL)
            a = lhs(at)
            for i in range(2):
                v = jnp.dot(a, wv[slot, i, at, :], preferred_element_type=F32)
                out[i] = v if k == 0 else out[i] + v
            for when, act in beside:
                if when == k:
                    act()
        return out

    late = 3 * (K // COL) // 4

    def gate_up(m, t, hs, j, waits, *beside):
        g, u = products(lambda at: xv[pl.ds(0, m), at], t, waits, beside)
        hv[hs, pl.ds(0, m), pl.ds(pl.multiple_of(j * COL, COL), COL)] = (jax.nn.silu(g) * u).astype(BF16)

    def down_pair(t, hs, c, q, beside):
        s = lax.rem(c * drounds + q, lag)
        came = lax.rem(jnp.maximum(c * rsn + q - lag, 0), ring)
        place = jnp.where(q >= lag, came, ring)

        def ready():
            for way in range(2):
                @pl.when(c * drounds + q >= lag)
                def _():
                    rs_copy(way, s, 0).wait_send()

                @pl.when((c >= 1) & (q < lag))
                def _():
                    y_own(way, s, 0, 0).wait()

                @pl.when(q >= lag)
                def _():
                    rs_copy(way, 0, came).wait_recv()

        for k in range(2):
            both = products(lambda at: hv[hs, :, at], t + k, 2 - 2 * k, [ready] if k == 0 else beside)
            at = pl.ds(k * COL, COL)
            for way in range(2):
                v = both[way] + rsin[way, place, :, at].astype(F32)
                stg[way, s, :, at] = v.astype(BF16)

    def send(c, q):
        s = lax.rem(c * drounds + q, lag)
        slot = lax.rem(c * rsn + q, ring)
        for way in range(2):
            @pl.when(q < rsn)
            def _():
                rs_copy(way, s, slot).start()

            @pl.when(q >= rsn)
            def _():
                ag_first(way, s, c, q - rsn).start()

            @pl.when(q >= rsn)
            def _():
                y_own(way, s, c, q - rsn).start()

    w_start(jnp.int32(0))
    x_copy(0, large).start()
    barrier = pltpu.get_barrier_semaphore()
    for other in (left, right):
        pl.semaphore_signal(barrier, inc=1, device_id={"tp": other}, device_id_type=MESH)
    pl.semaphore_wait(barrier, 2)
    w_start(jnp.int32(1))
    rsin[:, ring] = jnp.zeros_like(rsin[:, ring])
    x_copy(0, large).wait()
    w_wait(jnp.int32(0))
    w_start(jnp.int32(2))

    first, each = gn // 4, phase // 4

    def large_steps(v, _):
        i = jnp.where(v < first, 0, 1 + (v - first) // each)
        z = jnp.where(v < first, v + drounds, lax.rem(jnp.maximum(v - first, 0), each))
        t = 4 * v
        hs = lax.rem(i, 2)

        @pl.when(z < drounds)
        def _():
            @pl.when(z == 0)
            def _():
                x_copy(pl.multiple_of(i * large, 16), large).start()

            def x_wait():
                pl.when(z == 0)(lambda: x_copy(0, large).wait())

            down_pair(t, 1 - hs, i - 1, z, [x_wait])
            gate_up(large, t + 2, hs, 2 * z, 2, lambda: send(i - 1, z))
            gate_up(large, t + 3, hs, 2 * z + 1, 0)

        @pl.when(z >= drounds)
        def _():
            j = jnp.where(v < first, 4 * v, 4 * z - dn)
            ev = z - drounds
            on = (v >= first) & (ev < (nt - 2) * lag)
            gate_up(large, t, hs, j, 2, lambda: forward(i - 1, ev, on))
            for k in range(1, 4):
                gate_up(large, t + k, hs, j + k, 2 if k == 2 else 0)

        return 0

    lax.fori_loop(0, first + each * (count - 1), large_steps, 0)

    t0, c0 = gn + (count - 1) * phase, count - 1
    hs0, hs1 = c0 % 2, count % 2
    x_copy(count * large, small).start()

    def mixed_steps(q, _):
        t = t0 + 3 * q

        def x_wait():
            pl.when(q == 0)(lambda: x_copy(0, small).wait())

        down_pair(t, hs0, c0, q, [x_wait])
        gate_up(small, t + 2, hs1, q, 1, lambda: send(c0, q))
        return 0

    lax.fori_loop(0, drounds, mixed_steps, 0)

    def small_steps(n, _):
        j = drounds + 2 * n
        on = (lax.rem(n, 3) == 0) & (n // 3 < (nt - 2) * lag)
        gate_up(small, t0 + dn + j, hs1, j, 1, lambda: forward(c0, n // 3, on))
        gate_up(small, t0 + dn + j + 1, hs1, j + 1, 1)
        return 0

    lax.fori_loop(0, (gn - drounds) // 2, small_steps, 0)

    t0 += phase

    def last_steps(ds, _):
        q, h = ds // 2, lax.rem(ds, 2)
        s = lax.rem(count * drounds + q, lag)
        came = lax.rem(count * rsn + jnp.maximum(q - lag, 0), ring)
        place = jnp.where(ds >= nb, came, ring)

        def ready():
            for way in range(2):
                @pl.when((q < lag) & (h == 0))
                def _():
                    rs_copy(way, s, 0).wait_send()
                    y_own(way, s, 0, 0).wait()

                @pl.when(ds >= nb)
                def _():
                    small_rs(way, s, h, 0).wait_send()

                @pl.when(ds >= nb)
                def _():
                    small_rs(way, 0, h, came).wait_recv()

        both = products(lambda at: hv[hs1, pl.ds(0, small), at], t0 + ds, 1, [ready])
        for way in range(2):
            v = both[way] + rsin[way, place, pl.ds(0, small), half(h)].astype(F32)
            stg[way, s, pl.ds(0, small), half(h)] = v.astype(BF16)
        slot, b = lax.rem(count * rsn + q, ring), ds - 2 * rsn

        @pl.when(ds < 2 * rsn)
        def _():
            for way in range(2):
                small_rs(way, s, h, slot).start()

        @pl.when(ds >= 2 * rsn)
        def _():
            for way in range(2):
                small_first(way, s, h, b).start()
                small_own(way, s, h, b).start()

        return 0

    lax.fori_loop(0, dn, last_steps, 0)

    for n in range(count * lag):
        for way in range(2):
            ag_copy(way, hops, n // lag, n % lag, 0, hops - 1).wait_recv()

    def keep(b):
        src = y.at[pl.ds(0, large * count), pl.ds(b * COL, COL)]
        return pltpu.make_async_copy(src, column(wv, b, large * count, rows), vsem.at[b])

    for b in range(y.shape[1] // COL):
        keep(b).start()

    for ev in range((nt - 2) * nb):
        hop, b = 1 + ev // nb, ev % nb
        for way in range(2):
            if ev >= nb:
                small_ag(way, 1, 0, b, 0).wait_send()
            small_ag(way, hop, b, b, hop - 1).wait_recv()
            small_ag(way, hop, b, b, hop).start()
    for way in range(2):
        for b in range(nb):
            small_rs(way, b // 2, b % 2, 0).wait_send()
            small_own(way, b // 2, b % 2, 0).wait()
            small_ag(way, 1, 0, b, 0).wait_send()
        for s in range(2):
            ag_copy(way, 1, 0, 0, s, 0).wait_send()
    for b in range(y.shape[1] // COL):
        keep(b).wait()
    for way in range(2):
        for b in range(nb):
            small_ag(way, hops, b, 0, hops - 1).wait_recv()


def column(v, b, rows, whole):
    per = v.shape[2] // whole
    return v.at[b // (2 * per), (b // per) % 2, pl.ds(b % per * whole, rows), :]


def lay_out(done, y, v, out, tail, sem, sems):
    rows, n = out.shape[0], out.shape[1] // COL
    rest = pltpu.make_async_copy(y.at[pl.ds(done, rows - done), :], tail, sem)
    rest.start()

    def copy(b):
        return pltpu.make_async_copy(column(v, b, done, rows), out.at[pl.ds(0, done), pl.ds(b * COL, COL)], sems.at[b])

    for b in range(n):
        copy(b).start()
    rest.wait()
    rest = pltpu.make_async_copy(tail, out.at[pl.ds(done, rows - done), :], sem)
    rest.start()
    for b in range(n):
        copy(b).wait()
    rest.wait()


def block(nt, large, count, x, wg, wu, wd):
    rows, K = x.shape
    nb = wd.shape[1] // (2 * nt * COL)
    lag = nb // 2
    assert wg.shape[1] == K and wd.shape[0] == K and wd.shape[1] == K and count * (nt - 2) * lag >= 2
    dma = pltpu.SemaphoreType.DMA
    y, v = pl.pallas_call(
        functools.partial(kernel, nt, large, count),
        out_shape=[jax.ShapeDtypeStruct((rows, wd.shape[1]), BF16), pltpu.VMEM((SLOTS, 2, K, COL), BF16)],
        in_specs=[pl.BlockSpec(memory_space=pl.ANY)] * 4,
        out_specs=[pl.BlockSpec(memory_space=pl.ANY), pl.BlockSpec(memory_space=pltpu.VMEM)],
        scratch_shapes=[
            pltpu.VMEM((large, K), BF16),
            pltpu.VMEM((2, large, K), BF16),
            pltpu.VMEM((2, 2 * lag + 1, large, WIDE), BF16),
            pltpu.VMEM((2, lag, large, WIDE), BF16),
            dma((SLOTS, 2)), dma,
            dma((2, lag)), dma((2, 2 * lag)), dma((2, nt - 1, count * lag)), dma((2, 2)), dma((2, lag)),
            dma((2, nb)), dma((2, 2 * nb)), dma((2, nt - 1, nb)), dma((2, nb)), dma((2, nb)), dma((wd.shape[1] // COL,)),
        ],
        compiler_params=pltpu.CompilerParams(collective_id=0, has_side_effects=True, vmem_limit_bytes=30 * 2**20),
        name="mlp_block",
    )(x, wg, wu, wd)
    return pl.pallas_call(
        functools.partial(lay_out, large * count),
        out_shape=jax.ShapeDtypeStruct((rows, wd.shape[1]), BF16),
        in_specs=[pl.BlockSpec(memory_space=pl.ANY)] * 2,
        out_specs=pl.BlockSpec(memory_space=pl.ANY),
        scratch_shapes=[pltpu.VMEM((rows - large * count, wd.shape[1]), BF16), dma, dma((wd.shape[1] // COL,))],
        compiler_params=pltpu.CompilerParams(vmem_limit_bytes=8 * 2**20),
        name="lay_out",
    )(pltpu.with_memory_space_constraint(y, pltpu.HBM), pltpu.with_memory_space_constraint(v, pltpu.VMEM))


def solution(mesh):
    nt = mesh.shape["tp"]
    return jax.shard_map(
        functools.partial(block, nt, LARGE, COUNT),
        mesh=mesh,
        in_specs=(P("dp", None), P(None, "tp"), P(None, "tp"), P("tp", None)),
        out_specs=P("dp", None),
        check_vma=False,
    )
```
